32 devices in a mesh: rep: 2 (over x), dp: 16 (over y, z, core).
Axes of the slice: x: 2, y: 2, z: 4, core: 2. Of those that a mesh axis runs over, the one named last changes fastest.
Arguments:
- x: bfloat16 [32, 2048, 640], P(('rep', 'dp')), parts along dimension 0
- dy: bfloat16 [32, 2048, 640], P(('rep', 'dp')), parts along dimension 0
- wq: bfloat16 [2, 640, 512], P(None, 'dp')
- wk: bfloat16 [2, 640, 256], P(None, 'dp')
- wv: bfloat16 [2, 640, 256], P(None, 'dp')
- wo: bfloat16 [2, 512, 640], P(None, 'dp')
- w_gate: bfloat16 [2, 640, 2560], P(None, 'dp')
- w_up: bfloat16 [2, 640, 2560], P(None, 'dp')
- w_down: bfloat16 [2, 2560, 640], P(None, 'dp')
- m_wq: float32 [2, 640, 512], P(None, 'dp')
- m_wk: float32 [2, 640, 256], P(None, 'dp')
- m_wv: float32 [2, 640, 256], P(None, 'dp')
- m_wo: float32 [2, 512, 640], P(None, 'dp')
- m_w_gate: float32 [2, 640, 2560], P(None, 'dp')
- m_w_up: float32 [2, 640, 2560], P(None, 'dp')
- m_w_down: float32 [2, 2560, 640], P(None, 'dp')
- v_wq: float32 [2, 640, 512], P(None, 'dp')
- v_wk: float32 [2, 640, 256], P(None, 'dp')
- v_wv: float32 [2, 640, 256], P(None, 'dp')
- v_wo: float32 [2, 512, 640], P(None, 'dp')
- v_w_gate: float32 [2, 640, 2560], P(None, 'dp')
- v_w_up: float32 [2, 640, 2560], P(None, 'dp')
- v_w_down: float32 [2, 2560, 640], P(None, 'dp')
Outputs:
- output 1: bfloat16 [4, 640, 512], P('rep', 'dp'), parts along dimension 0
- output 2: bfloat16 [4, 640, 256], P('rep', 'dp'), parts along dimension 0
- output 3: bfloat16 [4, 640, 256], P('rep', 'dp'), parts along dimension 0
- output 4: bfloat16 [4, 512, 640], P('rep', 'dp'), parts along dimension 0
- output 5: bfloat16 [4, 640, 2560], P('rep', 'dp'), parts along dimension 0
- output 6: bfloat16 [4, 640, 2560], P('rep', 'dp'), parts along dimension 0
- output 7: bfloat16 [4, 2560, 640], P('rep', 'dp'), parts along dimension 0
- output 8: float32 [4, 640, 512], P('rep', 'dp'), parts along dimension 0
- output 9: float32 [4, 640, 256], P('rep', 'dp'), parts along dimension 0
- output 10: float32 [4, 640, 256], P('rep', 'dp'), parts along dimension 0
- output 11: float32 [4, 512, 640], P('rep', 'dp'), parts along dimension 0
- output 12: float32 [4, 640, 2560], P('rep', 'dp'), parts along dimension 0
- output 13: float32 [4, 640, 2560], P('rep', 'dp'), parts along dimension 0
- output 14: float32 [4, 2560, 640], P('rep', 'dp'), parts along dimension 0
- output 15: float32 [4, 640, 512], P('rep', 'dp'), parts along dimension 0
- output 16: float32 [4, 640, 256], P('rep', 'dp'), parts along dimension 0
- output 17: float32 [4, 640, 256], P('rep', 'dp'), parts along dimension 0
- output 18: float32 [4, 512, 640], P('rep', 'dp'), parts along dimension 0
- output 19: float32 [4, 640, 2560], P('rep', 'dp'), parts along dimension 0
- output 20: float32 [4, 640, 2560], P('rep', 'dp'), parts along dimension 0
- output 21: float32 [4, 2560, 640], P('rep', 'dp'), parts along dimension 0
There are 2 independent parts. The reference program is written for one: setup_inputs(seed, part) draws one part's arguments, and reference() takes and returns one part's arrays. A program takes and returns all parts, laid end to end along the dimension named above; an argument that names none is the same for every part.
All inputs are finite; a program needn't handle non-finite values.
Results may differ from the reference program's by a relative error of at most 0.0273.
Values are sent between devices in bfloat16 or wider.
A program may use at most 2 GiB of HBM per device.

```python
import jax
import jax.numpy as jnp
from jax import lax

SEQUENCES = 16
TOKENS = 2048
D = 640
HEADS = 2
KV_HEADS = 1
HEAD = 256
FF = 2560
LAYERS = 2
THETA = 10000
NAMES = ("wq", "wk", "wv", "wo", "w_gate", "w_up", "w_down")
SHAPES = {
    "wq": (LAYERS, D, HEADS * HEAD),
    "wk": (LAYERS, D, KV_HEADS * HEAD),
    "wv": (LAYERS, D, KV_HEADS * HEAD),
    "wo": (LAYERS, HEADS * HEAD, D),
    "w_gate": (LAYERS, D, FF),
    "w_up": (LAYERS, D, FF),
    "w_down": (LAYERS, FF, D),
}


def bump(key, n, height):
    away = (jnp.arange(n, dtype=jnp.int32) - jax.random.randint(key, (), 0, n, jnp.int32)) % n
    return jnp.where(away < n // 8, height, 1.0)


def together(key, own, strength):
    shared = jax.random.normal(key, own.shape[1:], jnp.float32)
    return (own + strength * shared) * lax.rsqrt(1 + strength * strength)


def setup_inputs(seed: int = 0, part: int = 0) -> dict:
    kx, kdy, ka, kb, kz, kf, kh, kl, *keys = jax.random.split(jax.random.key(seed), 8 + 3 * len(NAMES))
    kx, kdy, ka, kb = (jax.random.fold_in(k, part) for k in (kx, kdy, ka, kb))
    kw, km, kv = (keys[i::3] for i in range(3))
    shape = (SEQUENCES, TOKENS, D)
    much_x, much_dy = jax.random.uniform(kz, (2,), jnp.float32, 0.0, 1.0)
    loud = 2.0 ** jax.random.uniform(jax.random.fold_in(kz, 1), (), jnp.float32, -1.0, 2.0)
    layers = 2.0 ** jax.random.uniform(kl, (LAYERS, 1, 1), jnp.float32, -1.0, 1.0)
    times = {"wq": 1.0, "wk": 1.0, "wv": 2.0, "wo": layers, "w_gate": 1.0, "w_up": bump(kh, FF, 4.0), "w_down": layers}
    x = together(ka, jax.random.normal(kx, shape, jnp.float32), much_x) * bump(kf, D, 4.0)
    dy = together(kb, jax.random.normal(kdy, shape, jnp.float32), much_dy)
    drawn = {"x": x.astype(jnp.bfloat16), "dy": (loud * dy * (SEQUENCES * TOKENS) ** -0.5).astype(jnp.bfloat16)}
    for key, name in zip(kw, NAMES, strict=True):
        drawn[name] = (jax.random.normal(key, SHAPES[name], jnp.float32) * SHAPES[name][1] ** -0.5 * times[name]).astype(jnp.bfloat16)
    for key, name in zip(km, NAMES, strict=True):
        drawn[f"m_{name}"] = 0.1 * jax.random.normal(key, SHAPES[name], jnp.float32)
    for key, name in zip(kv, NAMES, strict=True):
        drawn[f"v_{name}"] = loud * loud * jax.random.uniform(key, SHAPES[name], jnp.float32, 0.2, 0.6)
    return drawn


def matmul(a, w):
    return jnp.dot(a, w, preferred_element_type=jnp.float32).astype(jnp.bfloat16)


def normed(h):
    wide = h.astype(jnp.float32)
    scale = lax.rsqrt(jnp.mean(wide**2, -1, keepdims=True) + 1e-6)
    return (wide * scale).astype(jnp.bfloat16)


def turned(t, theta):
    half = t.shape[-1] // 2
    angle = jnp.arange(t.shape[0], dtype=jnp.float32)[:, None] * theta ** (-jnp.arange(half, dtype=jnp.float32) / half)
    cos, sin = jnp.cos(angle)[:, None], jnp.sin(angle)[:, None]
    a, b = t[..., :half].astype(jnp.float32), t[..., half:].astype(jnp.float32)
    return jnp.concatenate([a * cos - b * sin, b * cos + a * sin], -1).astype(jnp.bfloat16)


def seen_by(q, k, v):
    tokens, kv = q.shape[0], k.shape[1]
    q = q.reshape(tokens, kv, -1, q.shape[-1])
    scores = jnp.einsum("tgsd,ugd->gstu", q.astype(jnp.float32), k.astype(jnp.float32)) * q.shape[-1] ** -0.5
    place = jnp.arange(tokens)
    weights = jax.nn.softmax(jnp.where(place[:, None] >= place, scores, -jnp.inf), -1).astype(jnp.bfloat16)
    return jnp.einsum("gstu,ugd->tgsd", weights.astype(jnp.float32), v.astype(jnp.float32)).astype(jnp.bfloat16).reshape(tokens, -1)


def layer(h, w):
    a = normed(h)
    q, k = (turned(matmul(a, w[name]).reshape(h.shape[0], -1, HEAD), THETA) for name in ("wq", "wk"))
    h = h + matmul(seen_by(q, k, matmul(a, w["wv"]).reshape(h.shape[0], -1, HEAD)), w["wo"])
    b = normed(h)
    gate = jnp.dot(b, w["w_gate"], preferred_element_type=jnp.float32)
    up = jnp.dot(b, w["w_up"], preferred_element_type=jnp.float32)
    return h + matmul((jax.nn.silu(gate) * up).astype(jnp.bfloat16), w["w_down"])


def adamw(w, m, v, g):
    m = 0.9 * m + 0.1 * g
    v = 0.95 * v + 0.05 * g * g
    step = m * lax.rsqrt(v + 1e-8) + 0.1 * w
    return (w - 0.02 * step).astype(jnp.bfloat16), m, v


def stack(weights, h):
    return lax.scan(lambda h, w: (layer(h, w), None), h, weights)[0]


def reference(x, dy, wq, wk, wv, wo, w_gate, w_up, w_down, m_wq, m_wk, m_wv, m_wo, m_w_gate, m_w_up, m_w_down, v_wq, v_wk, v_wv, v_wo, v_w_gate, v_w_up, v_w_down):
    weights = dict(zip(NAMES, (wq, wk, wv, wo, w_gate, w_up, w_down), strict=True))

    def take(so_far, sequence):
        h, by_y = sequence
        _, back = jax.vjp(stack, weights, h)
        by_weights, by_h = back(by_y)
        return jax.tree.map(lambda total, term: total + term.astype(jnp.float32), so_far, by_weights), by_h

    none_yet = {name: jnp.zeros(w.shape, jnp.float32) for name, w in weights.items()}
    by_weights, by_x = lax.scan(take, none_yet, (x, dy))
    gradients = [by_weights[name].astype(jnp.bfloat16).astype(jnp.float32) for name in NAMES]
    first = (m_wq, m_wk, m_wv, m_wo, m_w_gate, m_w_up, m_w_down)
    second = (v_wq, v_wk, v_wv, v_wo, v_w_gate, v_w_up, v_w_down)
    new = [adamw(weights[name].astype(jnp.float32), m, v, g) for name, m, v, g in zip(NAMES, first, second, gradients, strict=True)]
    return tuple(one[which] for which in range(3) for one in new)
```

```python
import functools

import jax
import jax.numpy as jnp
from jax import lax
from jax.experimental import pallas as pl
from jax.experimental.pallas import tpu as pltpu
from jax.sharding import PartitionSpec as P

HEAD = 256
HEADS = 2
THETA = 10000
NAMES = ("wq", "wk", "wv", "wo", "w_gate", "w_up", "w_down")
FFN = NAMES[4:]
BF, F32 = jnp.bfloat16, jnp.float32
NEG = -1e30
HIDDEN = 2 * NEG
LOG2E = 1.4426950408889634
VMEM = 58 * 2**20
CHUNK = 512
BLOCK = 512
MESH = pl.DeviceIdType.MESH
ANY = pl.BlockSpec(memory_space=pl.ANY)
IN_VMEM = pl.BlockSpec(memory_space=pltpu.VMEM)


def _dot(a, b, ca, cb):
    return lax.dot_general(a, b, (((ca,), (cb,)), ((), ())), preferred_element_type=F32)


def _whole(x):
    return pl.BlockSpec(x.shape, lambda i: (0,) * len(x.shape))


def _rows(width):
    return pl.BlockSpec((BLOCK, width), lambda i: (i, 0))


def _heads(n):
    return pl.BlockSpec((n, BLOCK, HEAD), lambda i: (0, i, 0))


def _stats():
    return pl.BlockSpec((HEADS, BLOCK), lambda i: (0, i))


def _like(*shape, dtype=BF):
    return jax.ShapeDtypeStruct(shape, dtype)


class Nothing:
    args, in_specs, out_specs, out_shape, scratch, number = (), (), (), (), (), None

    def bind(self, ins, outs, scratch):
        return {}, lambda: None


def _call(kernel, steps, args, in_specs, out_specs, out_shape, scratch=(), flops=0, beside=Nothing()):
    sizes = [len(args), len(beside.args), len(out_shape), len(beside.out_shape), len(scratch), len(beside.scratch)]

    def body(*refs):
        cut = []
        for size in sizes:
            cut.append(refs[:size])
            refs = refs[size:]
        i = pl.program_id(0)
        early, late = beside.bind(*cut[1::2])
        for at, work in early.items():
            pl.when(i == at)(work)
        kernel(i, *cut[0], *cut[2], *cut[4])
        if early:
            pl.when(i == steps - 1)(late)

    extra = {} if beside.number is None else dict(collective_id=beside.number, has_side_effects=True)
    arrays = [*args, *out_shape]
    got = pl.pallas_call(
        body,
        grid=(steps,),
        in_specs=[*in_specs, *beside.in_specs],
        out_specs=[*out_specs, *beside.out_specs],
        out_shape=[*out_shape, *beside.out_shape],
        scratch_shapes=[*scratch, *beside.scratch],
        compiler_params=pltpu.CompilerParams(dimension_semantics=("arbitrary",), vmem_limit_bytes=VMEM, **extra),
        cost_estimate=pl.CostEstimate(flops=flops, transcendentals=0, bytes_accessed=sum(a.size * a.dtype.itemsize for a in arrays)),
    )(*args, *beside.args)
    return (got[: len(out_shape)], beside.results(got[len(out_shape) :])) if beside.args else got


class Exchange:
    def __init__(self, arrays, number, plan):
        self.args, self.number, self.n = arrays, number, len(arrays)
        self.plan = plan

    def stages(self, begin, works, order, end):
        early, planned = {0: [begin]}, set()
        for at, which in self.plan.items():
            early[at] = early.get(at, []) + [functools.partial(works[name], i) for name, i in which]
            planned.update(which)
        left = [functools.partial(works[name], i) for name, i in order if 0 <= i < self.n and (name, i) not in planned]
        together = lambda all: lambda: [work() for work in all] and None
        return {at: together(all) for at, all in early.items()}, together([*left, end])

    def semaphores(self, copies):
        return [pltpu.SemaphoreType.DMA((self.n, copies)), pltpu.SemaphoreType.DMA((self.n, copies)), pltpu.SemaphoreType.DMA((self.n,))]

    def place(self):
        me = lax.axis_index("dp")
        self.me, self.y, self.z, self.c = me, me // 8, me // 2 % 4, me % 2
        self.core, self.across = me + 1 - 2 * self.c, (me + 8) % 16
        self.along = [self.y * 8 + (self.z + k) % 4 * 2 + self.c for k in (1, 2, 3)]

    def meet(self, more=()):
        barrier = pltpu.get_barrier_semaphore()
        others = [{"dp": one} for one in (self.core, self.across, *self.along)] + list(more)
        for other in others:
            pl.semaphore_signal(barrier, inc=1, device_id=other, device_id_type=MESH)
        pl.semaphore_wait(barrier, len(others))

    def remote(self, i, number, src, dst, to):
        return pltpu.make_async_remote_copy(src_ref=src, dst_ref=dst, send_sem=self.send.at[i, number], recv_sem=self.recv.at[i, number],
                                            device_id=to if isinstance(to, dict) else {"dp": to}, device_id_type=MESH)


class Gather(Exchange):
    def __init__(self, arrays, number, plan={}, halved=0):
        super().__init__(arrays, number, plan)
        self.halved = halved
        self.in_specs, self.out_specs = [IN_VMEM] * self.n, [ANY] * self.n
        self.out_shape = [_like(16, *x.shape) for x in arrays]
        self.scratch = self.semaphores(29)

    def results(self, got):
        return [x.reshape(-1, x.shape[2]) for x in got]

    def bind(self, xs, outs, scratch):
        self.send, self.recv, local = scratch
        self.place()
        y, z, c, me = self.y, self.z, self.c, self.me
        line = [y * 8 + (z + 4 - k) % 4 * 2 + c for k in range(4)]
        far = [(1 - y) * 8 + (z + 4 - k) % 4 * 2 + c for k in range(4)]
        other = 1 - 2 * c
        n, halved, sends = self.n, self.halved, []
        x = lax.axis_index("rep")
        twin = {"rep": 1 - x, "dp": me}

        def half(ref, i, which):
            if i >= halved or which is None:
                return ref
            width = self.args[i].shape[1] // 2
            return ref.at[:, pl.ds(pl.multiple_of(which * width, 128), width)]

        def copy(i, number, slot, to, which, own=False):
            block = half(outs[i].at[slot], i, which)
            return self.remote(i, number, half(xs[i], i, which) if own else block, block, to)

        def start(*args):
            sends.append(args)
            copy(*args).start()

        def kept(i):
            return pltpu.make_async_copy(xs[i], outs[i].at[me], local.at[i])

        def begin():
            self.meet([twin] if halved else [])
            for i in range(n):
                kept(i).start()
                for k in range(3):
                    start(i, k, me, self.along[k], x, True)
                start(i, 3, me, self.across, x, True)
                start(i, 7, me, self.core, None, True)

        def from_far(i):
            for k in range(4):
                copy(i, 3 + k, far[k], self.across, x).wait_recv()
                start(i, 11 + k, far[k], self.core, x)
                if i < halved:
                    start(i, 18 + k, far[k], twin, x)

        def from_twin(i):
            for k in range(7 * (i < halved)):
                slot = line[k + 1] if k < 3 else far[k - 3]
                copy(i, 15 + k, slot, twin, 1 - x).wait_recv()
                start(i, 22 + k, slot, self.core, 1 - x)

        def from_line(i):
            for k in (1, 2, 3):
                copy(i, k - 1, line[k], self.along[k - 1], x).wait_recv()
                start(i, 3 + k, line[k], self.across, x)
                start(i, 7 + k, line[k], self.core, x)
                if i < halved:
                    start(i, 14 + k, line[k], twin, x)

        def end():
            for i in range(n):
                copy(i, 7, line[0] + other, self.core, None).wait_recv()
                for k in range(7):
                    slot = (line[k + 1] if k < 3 else far[k - 3]) + other
                    copy(i, 8 + k, slot, self.core, x).wait_recv()
                    if i < halved:
                        copy(i, 22 + k, slot, self.core, 1 - x).wait_recv()
                kept(i).wait()
            for args in sends:
                copy(*args).wait_send()

        order = [(name, i - late) for i in range(n + 2) for late, name in enumerate(("line", "far", "twin"))]
        return self.stages(begin, dict(line=from_line, far=from_far, twin=from_twin), order, end)


class Scatter(Exchange):
    def __init__(self, gradients, number, plan={}):
        arrays = [g.reshape(8, 2, g.shape[0] // 16, g.shape[1]) for g in gradients]
        super().__init__(arrays, number, plan)
        self.in_specs, self.out_specs = [ANY] * self.n, [IN_VMEM] * self.n
        self.out_shape = [_like(*g.shape[2:]) for g in arrays]
        self.scratch = [pltpu.VMEM((blocks, *g.shape[2:]), BF) for g in arrays for blocks in (8, 8, 4, 3)] + self.semaphores(5)

    def results(self, got):
        return got

    def bind(self, gs, outs, scratch):
        self.send, self.recv, local = scratch[-3:]
        buffers = [scratch[4 * i : 4 * i + 4] for i in range(self.n)]
        self.place()
        y, z, c = self.y, self.z, self.c
        places = [(z + k) % 4 for k in range(4)]
        n = self.n

        def kept(i):
            return pltpu.make_async_copy(gs[i].at[:, c], buffers[i][0], local.at[i])

        def to_core(i):
            return self.remote(i, 0, gs[i].at[:, 1 - c], buffers[i][1], self.core)

        def to_far(i):
            return self.remote(i, 1, buffers[i][0].at[pl.ds((1 - y) * 4, 4)], buffers[i][2], self.across)

        def to_line(i, k):
            return self.remote(i, 2 + k, buffers[i][0].at[y * 4 + places[k + 1]], buffers[i][3].at[k], self.along[k])

        def begin():
            self.meet()
            for i in range(n):
                to_core(i).start()
                kept(i).start()

        def one(i):
            own, a = buffers[i][:2]
            kept(i).wait()
            to_core(i).wait_recv()

            @pl.loop(0, 4)
            def _(q):
                at = (1 - y) * 4 + q
                own[at] = (own[at].astype(F32) + a[at].astype(F32)).astype(BF)

            to_far(i).start()

        def so_far(i, at):
            own, a, b, _ = buffers[i]
            return own[y * 4 + at].astype(F32) + a[y * 4 + at].astype(F32) + b[at].astype(F32)

        def two(i):
            to_far(i).wait_recv()
            for k in range(3):
                buffers[i][0][y * 4 + places[k + 1]] = so_far(i, places[k + 1]).astype(BF)
                to_line(i, k).start()

        def end():
            for i in range(n):
                for k in range(3):
                    to_line(i, k).wait_recv()
                outs[i][...] = sum((buffers[i][3][k].astype(F32) for k in range(3)), so_far(i, z)).astype(BF)
            for i in range(n):
                to_core(i).wait_send()
                to_far(i).wait_send()
                for k in range(3):
                    to_line(i, k).wait_send()

        order = [(name, i - late) for i in range(n + 1) for late, name in enumerate(("one", "two"))]
        return self.stages(begin, dict(one=one, two=two), order, end)


def alone(exchange):
    return _call(lambda i: None, 1, (), (), (), (), flops=10**9, beside=exchange)[1]


def _scale(wide):
    return lax.rsqrt(jnp.mean(wide * wide, -1, keepdims=True) + 1e-6)


def _norm(h):
    wide = h.astype(F32)
    return (wide * _scale(wide)).astype(BF)


def _norm_back(h, by_out):
    wide, by_out = h.astype(F32), by_out.astype(BF).astype(F32)
    s = _scale(wide)
    return by_out * s - wide * (s * s * s * jnp.mean(wide * by_out, -1, keepdims=True))


def _add(h, more):
    return (h.astype(F32) + more.astype(BF).astype(F32)).astype(BF)


def _turn(t, cos, sin):
    half = HEAD // 2
    a, b = t[:, :half].astype(F32), t[:, half:].astype(F32)
    return jnp.concatenate([a * cos - b * sin, b * cos + a * sin], -1).astype(BF)


def _part(n):
    return slice(n * HEAD, (n + 1) * HEAD)


def enter(h, w, tables):
    tokens, d = h.shape

    def kernel(i, h_ref, w_ref, cos_ref, sin_ref, q_ref, k_ref, v_ref):
        t = _dot(_norm(h_ref[...]), w_ref[...], 1, 0).astype(BF)
        cos, sin = cos_ref[...], sin_ref[...]
        for n in range(HEADS):
            q_ref[n] = _turn(t[:, _part(n)], cos, sin)
        k_ref[0] = _turn(t[:, _part(HEADS)], cos, sin)
        v_ref[0] = t[:, _part(HEADS + 1)]

    return _call(kernel, tokens // BLOCK, (h, w, *tables), [_rows(d), _whole(w), *[_rows(HEAD // 2)] * 2], [_heads(HEADS), _heads(1), _heads(1)],
                 [_like(n, tokens, HEAD) for n in (HEADS, 1, 1)], flops=2 * tokens * w.size)


def _gap(columns):
    shape = (BLOCK, columns)
    return lax.rem(lax.broadcasted_iota(jnp.int32, shape, 1), BLOCK) - lax.broadcasted_iota(jnp.int32, shape, 0)


def attend(q, k, v, beside):
    tokens = q.shape[1]
    columns = HEADS * BLOCK
    scale = HEAD**-0.5
    e = scale * LOG2E

    def kernel(i, q_ref, k_ref, v_ref, o_ref, lse_ref, top_s, mix_s):
        top_s[...] = jnp.full(top_s.shape, NEG, F32)
        mix_s[...] = jnp.zeros(mix_s.shape, F32)
        ones = jnp.ones((8, BLOCK), BF)

        def block(j, masked):
            here = pl.ds(pl.multiple_of(j * BLOCK, BLOCK), BLOCK)
            keys = k_ref[0, here, :]
            scores = [_dot(keys, q_ref[n], 1, 1) for n in range(HEADS)]
            weights, keeps = [], []
            for n, s in enumerate(scores):
                at = slice(n * BLOCK, (n + 1) * BLOCK)
                if masked:
                    s = jnp.where(_gap(BLOCK) >= 0, s, HIDDEN)
                old = top_s[:, at]
                top = jnp.maximum(old, s.max(axis=0, keepdims=True))
                top_s[:, at] = top
                weights.append(jnp.exp2((s - top) * e).astype(BF))
                keeps.append(jnp.exp2((old - top) * e))
            values = jnp.concatenate([v_ref[0, here, :].T, ones], axis=0)
            for n in range(HEADS):
                at = slice(n * BLOCK, (n + 1) * BLOCK)
                mix_s[:, at] = mix_s[:, at] * keeps[n] + _dot(values, weights[n], 1, 0)

        lax.fori_loop(0, i, lambda j, _: block(j, False), None)
        block(i, True)
        for n in range(HEADS):
            at = slice(n * BLOCK, (n + 1) * BLOCK)
            total = mix_s[HEAD : HEAD + 1, at]
            o_ref[n] = (mix_s[:HEAD, at] * (1 / total)).T.astype(BF)
            lse_ref[n : n + 1, :] = top_s[:, at] * scale + jnp.log(total)

    return _call(kernel, tokens // BLOCK, (q, k, v), [_heads(HEADS), _whole(k), _whole(v)], [_heads(HEADS), _stats()],
                 [_like(*q.shape), _like(HEADS, tokens, dtype=F32)], [pltpu.VMEM((1, columns), F32), pltpu.VMEM((HEAD + 8, columns), F32)],
                 flops=3 * tokens * q.size, beside=beside)


def attend_back(q, k, v, d_out, lse, delta, beside):
    tokens = q.shape[1]
    columns = HEADS * BLOCK
    scale = HEAD**-0.5
    e = scale * LOG2E
    steps = tokens // BLOCK

    def kernel(i, q_ref, k_ref, v_ref, do_ref, lse_ref, delta_ref, dq_ref, dk_ref, dv_ref, dq_s, dk_s, dv_s):
        @pl.when(i == 0)
        def _():
            dk_s[...] = jnp.zeros(dk_s.shape, F32)
            dv_s[...] = jnp.zeros(dv_s.shape, F32)

        dq_s[...] = jnp.zeros(dq_s.shape, F32)

        def block(j, masked):
            here = pl.ds(pl.multiple_of(j * BLOCK, BLOCK), BLOCK)
            keys, values = k_ref[0, here, :], v_ref[0, here, :]
            scores = [_dot(keys, q_ref[n], 1, 1) for n in range(HEADS)]
            dps = [_dot(values, do_ref[n], 1, 1) for n in range(HEADS)]
            for n in range(HEADS):
                at = slice(n * BLOCK, (n + 1) * BLOCK)
                p = jnp.exp2(scores[n] * e - lse_ref[n : n + 1, :] * LOG2E)
                if masked:
                    p = jnp.where(_gap(BLOCK) >= 0, p, 0.0)
                ds = (p * (dps[n] - delta_ref[n : n + 1, :])).astype(BF)
                dv_s[here, :] += _dot(p.astype(BF), do_ref[n], 1, 0)
                dk_s[here, :] += _dot(ds, q_ref[n], 1, 0)
                dq_s[:, at] += _dot(keys.T, ds, 1, 0)

        lax.fori_loop(0, i, lambda j, _: block(j, False), None)
        block(i, True)
        for n in range(HEADS):
            dq_ref[n] = (dq_s[:, n * BLOCK : (n + 1) * BLOCK] * scale).T.astype(BF)

        @pl.when(i == steps - 1)
        def _():
            dk_ref[0] = (dk_s[...] * scale).astype(BF)
            dv_ref[0] = dv_s[...].astype(BF)

    return _call(kernel, steps, (q, k, v, d_out, lse, delta), [_heads(HEADS), _whole(k), _whole(v), _heads(HEADS), _stats(), _stats()],
                 [_heads(HEADS), _whole(k), _whole(v)], [_like(*q.shape), _like(*k.shape), _like(*v.shape)],
                 [pltpu.VMEM((HEAD, columns), F32), pltpu.VMEM((tokens, HEAD), F32), pltpu.VMEM((tokens, HEAD), F32)],
                 flops=6 * tokens * q.size, beside=beside)


def leave(h, o, wo):
    def kernel(i, h_ref, o_ref, wo_ref, out_ref):
        out_ref[...] = _add(h_ref[...], sum(_dot(o_ref[n], wo_ref[_part(n), :], 1, 0) for n in range(HEADS)))

    tokens, d = h.shape
    return _call(kernel, tokens // BLOCK, (h, o, wo), [_rows(d), _heads(HEADS), _whole(wo)], [_rows(d)], [_like(*h.shape)], flops=2 * tokens * wo.size)[0]


def _feed_specs(d, chunk=CHUNK):
    return [*[pl.BlockSpec((d, chunk), lambda i: (0, i))] * 2, pl.BlockSpec((chunk, d), lambda i: (i, 0))]


def feed(h, gate, up, down, beside):
    tokens, d = h.shape
    steps = down.shape[0] // CHUNK

    def kernel(i, h_ref, gate_ref, up_ref, down_ref, out_ref, b_s, sum_s):
        @pl.when(i == 0)
        def _():
            b_s[...] = _norm(h_ref[...])
            sum_s[...] = jnp.zeros(sum_s.shape, F32)

        b = b_s[...]
        g = _dot(b, gate_ref[...], 1, 0)
        u = _dot(b, up_ref[...], 1, 0)
        sum_s[...] += _dot((g * jax.nn.sigmoid(g) * u).astype(BF), down_ref[...], 1, 0)

        @pl.when(i == steps - 1)
        def _():
            out_ref[...] = _add(h_ref[...], sum_s[...])

    return _call(kernel, steps, (h, gate, up, down), [_whole(h), *_feed_specs(d)], [_whole(h)], [_like(*h.shape)],
                 [pltpu.VMEM(h.shape, BF), pltpu.VMEM(h.shape, F32)], flops=6 * tokens * down.size, beside=beside)


def feed_back(h, dy, gate, up, down, beside, chunk=CHUNK):
    tokens, d = h.shape
    hidden = down.shape[0]
    steps = hidden // chunk

    def kernel(i, h_ref, dy_ref, gate_ref, up_ref, down_ref, dh_ref, dgate_ref, dup_ref, ddown_ref, b_s, bt_s, dyt_s, sum_s):
        @pl.when(i == 0)
        def _():
            b = _norm(h_ref[...])
            b_s[...] = b
            bt_s[...] = b.T
            dyt_s[...] = dy_ref[...].T
            sum_s[...] = jnp.zeros(sum_s.shape, F32)

        b = b_s[...]
        g = _dot(b, gate_ref[...], 1, 0)
        u = _dot(b, up_ref[...], 1, 0)
        by = _dot(dy_ref[...], down_ref[...], 1, 1).astype(BF).astype(F32)
        s = jax.nn.sigmoid(g)
        silu = g * s
        p = (silu * u).astype(BF)
        du = (by * silu).astype(BF)
        dg = (by * u * (s + silu * (1 - s))).astype(BF)
        sum_s[...] += _dot(dg, gate_ref[...], 1, 1) + _dot(du, up_ref[...], 1, 1)
        dgate_ref[...] = _dot(bt_s[...], dg, 1, 0).astype(BF)
        dup_ref[...] = _dot(bt_s[...], du, 1, 0).astype(BF)
        ddown_ref[...] = _dot(dyt_s[...], p, 1, 0).T.astype(BF)

        @pl.when(i == steps - 1)
        def _():
            dh_ref[...] = _add(dy_ref[...], _norm_back(h_ref[...], sum_s[...]))

    specs = _feed_specs(d, chunk)
    return _call(kernel, steps, (h, dy, gate, up, down), [_whole(h), _whole(h), *specs], [_whole(h), *specs],
                 [_like(*h.shape), _like(d, hidden), _like(d, hidden), _like(hidden, d)],
                 [pltpu.VMEM(h.shape, BF), pltpu.VMEM((d, tokens), BF), pltpu.VMEM((d, tokens), BF), pltpu.VMEM(h.shape, F32)],
                 flops=16 * tokens * down.size, beside=beside)


def leave_back(dh, o, wo):
    tokens, d = dh.shape
    steps = tokens // BLOCK

    def kernel(i, dh_ref, o_ref, wo_ref, do_ref, delta_ref, dwo_ref, sum_s):
        dh = dh_ref[...]
        for n in range(HEADS):
            rows = _part(n)
            do = _dot(dh, wo_ref[rows, :], 1, 1).astype(BF)
            do_ref[n] = do
            o = o_ref[n]
            each = do.astype(F32) * o.astype(F32)
            each = each[:, : HEAD // 2] + each[:, HEAD // 2 :]
            delta_ref[n : n + 1, :] = jnp.sum(each.T, axis=0, keepdims=True)
            sum_s[rows, :] = jnp.where(i == 0, 0.0, sum_s[rows, :]) + _dot(o.T, dh, 1, 0)

        @pl.when(i == steps - 1)
        def _():
            dwo_ref[...] = sum_s[...].astype(BF)

    return _call(kernel, steps, (dh, o, wo), [_rows(d), _heads(HEADS), _whole(wo)], [_heads(HEADS), _stats(), _whole(wo)],
                 [_like(*o.shape), _like(HEADS, tokens, dtype=F32), _like(*wo.shape)], [pltpu.VMEM(wo.shape, F32)], flops=4 * tokens * wo.size)


def enter_back(h, dq, dk, dv, tables, dh=None, w=None):
    tokens, d = h.shape
    steps = tokens // BLOCK
    through = dh is not None
    dw = _like(d, (HEADS + 2) * HEAD)

    def kernel(i, h_ref, dq_ref, dk_ref, dv_ref, cos_ref, sin_ref, *rest):
        *rest, dw_ref, sum_s = rest
        cos, sin = cos_ref[...], -sin_ref[...]
        dt = jnp.concatenate([*[_turn(dq_ref[n], cos, sin) for n in range(HEADS)], _turn(dk_ref[0], cos, sin), dv_ref[0]], axis=1)
        h = h_ref[...]
        sum_s[...] = jnp.where(i == 0, 0.0, sum_s[...]) + _dot(_norm(h).T, dt, 1, 0)
        if through:
            dh_ref, w_ref, out_ref = rest
            out_ref[...] = _add(dh_ref[...], _norm_back(h, _dot(dt, w_ref[...], 1, 1)))

        @pl.when(i == steps - 1)
        def _():
            dw_ref[...] = sum_s[...].astype(BF)

    more = ((dh, w), [_rows(d), _whole(dw)], [_rows(d)], [_like(*h.shape)]) if through else ((), [], [], [])
    return _call(kernel, steps, (h, dq, dk, dv, *tables, *more[0]), [_rows(d), _heads(HEADS), _heads(1), _heads(1), *[_rows(HEAD // 2)] * 2, *more[1]],
                 [*more[2], _whole(dw)], [*more[3], dw], [pltpu.VMEM(dw.shape, F32)], flops=(2 + 2 * through) * tokens * dw.size)


def adamw(w, m, v, g):
    m = 0.9 * m + 0.1 * g
    v = 0.95 * v + 0.05 * g * g
    step = m * lax.rsqrt(v + 1e-8) + 0.1 * w
    return (w - 0.02 * step).astype(BF), m, v


def solution(mesh):
    def step(x, dy, *arrays):
        weights, m, v = (dict(zip(NAMES, arrays[i : i + 7], strict=True)) for i in (0, 7, 14))
        tokens, d = x.shape[1:]
        sides = [weights[name].shape[2] for name in NAMES[:3]]
        entries = [jnp.concatenate([weights[name][n] for name in NAMES[:3]], 1) for n in range(2)]
        half = HEAD // 2
        angle = jnp.arange(tokens, dtype=F32)[:, None] * THETA ** (-jnp.arange(half, dtype=F32) / half)
        tables = jnp.cos(angle), jnp.sin(angle)

        h0 = x[0]
        entry0, wo0 = alone(Gather([entries[0], weights["wo"][0]], 0))
        q0, k0, v0 = enter(h0, entry0, tables)
        (o0, lse0), ffn0 = attend(q0, k0, v0, Gather([weights[name][0] for name in FFN], 1, {3: [("line", 0)]}, 2))
        gate0, up0, down0 = ffn0
        mid0 = leave(h0, o0, wo0)
        rest = Gather([*(weights[name][1] for name in FFN), entries[1], weights["wo"][1]], 2,
                      {2: [("line", 0)], 3: [("line", 1), ("far", 0)], 4: [("far", 1)]}, 2)
        (h1,), others = feed(mid0, gate0, up0, down0, rest)
        gate1, up1, down1, entry1, wo1 = others
        q1, k1, v1 = enter(h1, entry1, tables)
        o1, lse1 = attend(q1, k1, v1, Nothing())
        mid1 = leave(h1, o1, wo1)

        by, d_gate, d_up, d_down = feed_back(mid1, dy[0], gate1, up1, down1, Nothing())
        new = [{}, {"w_down": lax.psum_scatter(d_down, "dp", scatter_dimension=0, tiled=True)}]
        d_o, delta, d_wo1 = leave_back(by, o1, wo1)
        dq, dk, dv = attend_back(q1, k1, v1, d_o, lse1, delta, Nothing())
        by, d_entry1 = enter_back(h1, dq, dk, dv, tables, by, entry1)
        plan = {0: [("one", 0), ("one", 1)], 1: [("one", 2), ("one", 3)], 3: [("two", 0)], 6: [("two", 1)], 7: [("two", 2), ("two", 3)]}
        (by, *d_ffn), sums = feed_back(mid0, by, gate0, up0, down0, Scatter([d_gate, d_up, d_wo1, d_entry1], 5, plan), CHUNK // 2)
        new[1]["w_gate"], new[1]["w_up"], new[1]["wo"], entry_sum1 = sums
        d_o, delta, d_wo0 = leave_back(by, o0, wo0)
        (dq, dk, dv), sums = attend_back(q0, k0, v0, d_o, lse0, delta, Scatter(d_ffn, 3, {1: [("one", 0)], 2: [("one", 1)], 3: [("one", 2)]}))
        (d_entry0,) = enter_back(h0, dq, dk, dv, tables)
        new[0].update(zip(FFN, sums))
        new[0]["wo"], entry_sum0 = alone(Scatter([d_wo0, d_entry0], 4))

        for n, g in enumerate((entry_sum0, entry_sum1)):
            at = 0
            for name, size in zip(NAMES, sides):
                new[n][name] = g[:, at : at + size]
                at += size
        out = [adamw(weights[name].astype(F32), m[name], v[name], jnp.stack([one[name] for one in new]).astype(F32)) for name in NAMES]
        return tuple(one[which] for which in range(3) for one in out)

    states, cut = P(("rep", "dp"), None, None), P(None, "dp", None)
    return jax.shard_map(
        step,
        mesh=mesh,
        in_specs=(states, states) + (cut,) * 21,
        out_specs=(P("rep", "dp", None),) * 21,
        check_vma=False,
    )
```

```python
import functools

import jax
import jax.numpy as jnp
from jax import lax
from jax.experimental import pallas as pl
from jax.experimental.pallas import tpu as pltpu
from jax.sharding import PartitionSpec as P

HEAD = 256
HEADS = 2
THETA = 10000
NAMES = ("wq", "wk", "wv", "wo", "w_gate", "w_up", "w_down")
FFN = NAMES[4:]
BF, F32 = jnp.bfloat16, jnp.float32
NEG = -1e30
HIDDEN = 2 * NEG
LOG2E = 1.4426950408889634
VMEM = 58 * 2**20
CHUNK = 512
BLOCK = 512
MESH = pl.DeviceIdType.MESH
ANY = pl.BlockSpec(memory_space=pl.ANY)
IN_VMEM = pl.BlockSpec(memory_space=pltpu.VMEM)


def _dot(a, b, ca, cb):
    return lax.dot_general(a, b, (((ca,), (cb,)), ((), ())), preferred_element_type=F32)


def _whole(x):
    return pl.BlockSpec(x.shape, lambda i: (0,) * len(x.shape))


def _rows(width):
    return pl.BlockSpec((BLOCK, width), lambda i: (i, 0))


def _heads(n):
    return pl.BlockSpec((n, BLOCK, HEAD), lambda i: (0, i, 0))


def _stats():
    return pl.BlockSpec((HEADS, BLOCK), lambda i: (0, i))


def _like(*shape, dtype=BF):
    return jax.ShapeDtypeStruct(shape, dtype)


class Nothing:
    args, in_specs, out_specs, out_shape, scratch, number = (), (), (), (), (), None

    def bind(self, ins, outs, scratch):
        return {}, lambda: None


def _call(kernel, steps, args, in_specs, out_specs, out_shape, scratch=(), flops=0, beside=Nothing()):
    sizes = [len(args), len(beside.args), len(out_shape), len(beside.out_shape), len(scratch), len(beside.scratch)]

    def body(*refs):
        cut = []
        for size in sizes:
            cut.append(refs[:size])
            refs = refs[size:]
        i = pl.program_id(0)
        early, late = beside.bind(*cut[1::2])
        for at, work in early.items():
            pl.when(i == at)(work)
        kernel(i, *cut[0], *cut[2], *cut[4])
        if early:
            pl.when(i == steps - 1)(late)

    extra = {} if beside.number is None else dict(collective_id=beside.number, has_side_effects=True)
    arrays = [*args, *out_shape]
    got = pl.pallas_call(
        body,
        grid=(steps,),
        in_specs=[*in_specs, *beside.in_specs],
        out_specs=[*out_specs, *beside.out_specs],
        out_shape=[*out_shape, *beside.out_shape],
        scratch_shapes=[*scratch, *beside.scratch],
        compiler_params=pltpu.CompilerParams(dimension_semantics=("arbitrary",), vmem_limit_bytes=VMEM, **extra),
        cost_estimate=pl.CostEstimate(flops=flops, transcendentals=0, bytes_accessed=sum(a.size * a.dtype.itemsize for a in arrays)),
    )(*args, *beside.args)
    return (got[: len(out_shape)], beside.results(got[len(out_shape) :])) if beside.args else got


class Exchange:
    def __init__(self, arrays, number, plan):
        self.args, self.number = arrays, number
        self.plan = plan

    def cut(self, whole=()):
        self.parts = []
        for i, x in enumerate(self.args):
            rows, columns = x.shape[-2:]
            first = columns if i in whole or rows * columns < 40 * 1024 else -(-columns // 256) * 128
            self.parts += [(i, at, width) for at, width in ((0, first), (first, columns - first)) if width]
        self.n = len(self.parts)

    def stages(self, begin, works, order, end):
        early, planned = {0: [begin]}, set()
        for at, which in self.plan.items():
            early[at] = early.get(at, []) + [functools.partial(works[name], i) for name, i in which]
            planned.update(which)
        left = [functools.partial(works[name], i) for name, i in order if 0 <= i < self.n and (name, i) not in planned]
        together = lambda all: lambda: [work() for work in all].clear()
        return {at: together(all) for at, all in early.items()}, together([*left, end])

    def semaphores(self, copies):
        return [pltpu.SemaphoreType.DMA((self.n, copies))] * 2 + [pltpu.SemaphoreType.DMA((self.n,))]

    def place(self):
        me = lax.axis_index("dp")
        self.me, self.y, self.z, self.c = me, me // 8, me // 2 % 4, me % 2
        self.core, self.across = me + 1 - 2 * self.c, (me + 8) % 16
        self.along = [self.y * 8 + (self.z + k) % 4 * 2 + self.c for k in (1, 2, 3)]

    def meet(self, more=()):
        barrier = pltpu.get_barrier_semaphore()
        others = [{"dp": one} for one in (self.core, self.across, *self.along)] + list(more)
        for other in others:
            pl.semaphore_signal(barrier, inc=1, device_id=other, device_id_type=MESH)
        pl.semaphore_wait(barrier, len(others))

    def remote(self, i, number, src, dst, to):
        return pltpu.make_async_remote_copy(src_ref=src, dst_ref=dst, send_sem=self.send.at[i, number], recv_sem=self.recv.at[i, number],
                                            device_id=to if isinstance(to, dict) else {"dp": to}, device_id_type=MESH)


class Gather(Exchange):
    def __init__(self, arrays, number, plan={}, halved=0):
        super().__init__(arrays, number, plan)
        self.halved = halved
        self.cut(range(halved))
        self.in_specs, self.out_specs = [IN_VMEM] * len(arrays), [ANY] * len(arrays)
        self.out_shape = [_like(16, *x.shape) for x in arrays]
        self.scratch = self.semaphores(29)

    def results(self, got):
        return [x.reshape(-1, x.shape[2]) for x in got]

    def bind(self, xs, outs, scratch):
        self.send, self.recv, local = scratch
        self.place()
        y, z, c, me = self.y, self.z, self.c, self.me
        line = [y * 8 + (z + 4 - k) % 4 * 2 + c for k in range(4)]
        far = [(1 - y) * 8 + (z + 4 - k) % 4 * 2 + c for k in range(4)]
        other = 1 - 2 * c
        n, halved, sends = self.n, self.halved, []
        x = lax.axis_index("rep")
        twin = {"rep": 1 - x, "dp": me}

        def half(ref, i, which):
            _, at, width = self.parts[i]
            if i >= halved or which is None:
                return ref.at[:, pl.ds(at, width)]
            return ref.at[:, pl.ds(pl.multiple_of(which * (width // 2), 128), width // 2)]

        def copy(i, number, slot, to, which, own=False):
            array = self.parts[i][0]
            block = half(outs[array].at[slot], i, which)
            return self.remote(i, number, half(xs[array], i, which) if own else block, block, to)

        def start(*args):
            sends.append(args)
            copy(*args).start()

        def kept(i):
            array = self.parts[i][0]
            return pltpu.make_async_copy(half(xs[array], i, None), half(outs[array].at[me], i, None), local.at[i])

        def begin():
            self.meet([twin] if halved else [])
            for i in range(n):
                kept(i).start()
                for k in range(3):
                    start(i, k, me, self.along[k], x, True)
                start(i, 3, me, self.across, x, True)
                start(i, 7, me, self.core, None, True)

        def from_far(i):
            for k in range(4):
                copy(i, 3 + k, far[k], self.across, x).wait_recv()
                start(i, 11 + k, far[k], self.core, x)
                if i < halved:
                    start(i, 18 + k, far[k], twin, x)

        def from_twin(i):
            for k in range(7 * (i < halved)):
                slot = line[k + 1] if k < 3 else far[k - 3]
                copy(i, 15 + k, slot, twin, 1 - x).wait_recv()
                start(i, 22 + k, slot, self.core, 1 - x)

        def from_line(i):
            for k in (1, 2, 3):
                copy(i, k - 1, line[k], self.along[k - 1], x).wait_recv()
                start(i, 3 + k, line[k], self.across, x)
                start(i, 7 + k, line[k], self.core, x)
                if i < halved:
                    start(i, 14 + k, line[k], twin, x)

        def end():
            for i in range(n):
                copy(i, 7, line[0] + other, self.core, None).wait_recv()
                for k in range(7):
                    slot = (line[k + 1] if k < 3 else far[k - 3]) + other
                    copy(i, 8 + k, slot, self.core, x).wait_recv()
                    if i < halved:
                        copy(i, 22 + k, slot, self.core, 1 - x).wait_recv()
                kept(i).wait()
            for args in sends:
                copy(*args).wait_send()

        order = [(name, i - late) for i in range(n + 2) for late, name in enumerate(("line", "far", "twin"))]
        return self.stages(begin, dict(line=from_line, far=from_far, twin=from_twin), order, end)


class Scatter(Exchange):
    def __init__(self, gradients, number, plan={}):
        arrays = [g.reshape(8, 2, g.shape[0] // 16, g.shape[1]) for g in gradients]
        super().__init__(arrays, number, plan)
        self.cut()
        self.in_specs, self.out_specs = [ANY] * len(arrays), [IN_VMEM] * len(arrays)
        self.out_shape = [_like(*g.shape[2:]) for g in arrays]
        self.scratch = [pltpu.VMEM((blocks, arrays[i].shape[2], width), BF) for i, _, width in self.parts for blocks in (8, 8, 4, 3)] + self.semaphores(5)

    def results(self, got):
        return got

    def bind(self, gs, outs, scratch):
        self.send, self.recv, local = scratch[-3:]
        buffers = [scratch[4 * i : 4 * i + 4] for i in range(self.n)]
        self.place()
        y, z, c = self.y, self.z, self.c
        places = [(z + k) % 4 for k in range(4)]
        n = self.n

        def terms(i, core):
            array, at, width = self.parts[i]
            return gs[array].at[:, core, :, pl.ds(at, width)]

        def kept(i):
            return pltpu.make_async_copy(terms(i, c), buffers[i][0], local.at[i])

        def to_core(i):
            return self.remote(i, 0, terms(i, 1 - c), buffers[i][1], self.core)

        def to_far(i):
            return self.remote(i, 1, buffers[i][0].at[pl.ds((1 - y) * 4, 4)], buffers[i][2], self.across)

        def to_line(i, k):
            return self.remote(i, 2 + k, buffers[i][0].at[y * 4 + places[k + 1]], buffers[i][3].at[k], self.along[k])

        def begin():
            self.meet()
            for i in range(n):
                to_core(i).start()
                kept(i).start()

        def one(i):
            own, a = buffers[i][:2]
            kept(i).wait()
            to_core(i).wait_recv()

            @pl.loop(0, 4)
            def _(q):
                at = (1 - y) * 4 + q
                own[at] = (own[at].astype(F32) + a[at].astype(F32)).astype(BF)

            to_far(i).start()

        def so_far(i, at):
            own, a, b, _ = buffers[i]
            return own[y * 4 + at].astype(F32) + a[y * 4 + at].astype(F32) + b[at].astype(F32)

        def two(i):
            to_far(i).wait_recv()
            for k in range(3):
                buffers[i][0][y * 4 + places[k + 1]] = so_far(i, places[k + 1]).astype(BF)
                to_line(i, k).start()

        def end():
            for i in range(n):
                for k in range(3):
                    to_line(i, k).wait_recv()
                array, at, width = self.parts[i]
                outs[array][:, at : at + width] = sum((buffers[i][3][k].astype(F32) for k in range(3)), so_far(i, z)).astype(BF)
            for i in range(n):
                to_core(i).wait_send()
                to_far(i).wait_send()
                for k in range(3):
                    to_line(i, k).wait_send()

        order = [(name, i - late) for i in range(n + 1) for late, name in enumerate(("one", "two"))]
        return self.stages(begin, dict(one=one, two=two), order, end)


def turning(tokens, beside):
    half = HEAD // 2
    pace = (THETA ** (-jnp.arange(half, dtype=F32) / half))[None]

    def kernel(i, pace_ref, cos_ref, sin_ref):
        angle = lax.broadcasted_iota(jnp.int32, (tokens, half), 0).astype(F32) * pace_ref[...]
        cos_ref[...] = jnp.cos(angle)
        sin_ref[...] = jnp.sin(angle)

    table = _like(tokens, half, dtype=F32)
    return _call(kernel, 1, (pace,), [_whole(pace)], [_whole(table)] * 2, [table] * 2, flops=10**9, beside=beside)


def alone(exchange):
    return _call(lambda i: None, 1, (), (), (), (), flops=10**9, beside=exchange)[1]


def _scale(wide):
    return lax.rsqrt(jnp.mean(wide * wide, -1, keepdims=True) + 1e-6)


def _norm(h):
    wide = h.astype(F32)
    return (wide * _scale(wide)).astype(BF)


def _norm_back(h, by_out):
    wide, by_out = h.astype(F32), by_out.astype(BF).astype(F32)
    s = _scale(wide)
    return by_out * s - wide * (s * s * s * jnp.mean(wide * by_out, -1, keepdims=True))


def _add(h, more):
    return (h.astype(F32) + more.astype(BF).astype(F32)).astype(BF)


def _turn(t, cos, sin):
    half = HEAD // 2
    a, b = t[:, :half].astype(F32), t[:, half:].astype(F32)
    return jnp.concatenate([a * cos - b * sin, b * cos + a * sin], -1).astype(BF)


def _part(n):
    return slice(n * HEAD, (n + 1) * HEAD)


def enter(h, w, tables):
    tokens, d = h.shape

    def kernel(i, h_ref, w_ref, cos_ref, sin_ref, q_ref, k_ref, v_ref):
        t = _dot(_norm(h_ref[...]), w_ref[...], 1, 0).astype(BF)
        cos, sin = cos_ref[...], sin_ref[...]
        for n in range(HEADS):
            q_ref[n] = _turn(t[:, _part(n)], cos, sin)
        k_ref[0] = _turn(t[:, _part(HEADS)], cos, sin)
        v_ref[0] = t[:, _part(HEADS + 1)]

    return _call(kernel, tokens // BLOCK, (h, w, *tables), [_rows(d), _whole(w), *[_rows(HEAD // 2)] * 2], [_heads(HEADS), _heads(1), _heads(1)],
                 [_like(n, tokens, HEAD) for n in (HEADS, 1, 1)], flops=2 * tokens * w.size)


def _gap(columns):
    shape = (BLOCK, columns)
    return lax.rem(lax.broadcasted_iota(jnp.int32, shape, 1), BLOCK) - lax.broadcasted_iota(jnp.int32, shape, 0)


def attend(q, k, v, beside):
    tokens = q.shape[1]
    columns = HEADS * BLOCK
    scale = HEAD**-0.5
    e = scale * LOG2E

    def kernel(i, q_ref, k_ref, v_ref, o_ref, lse_ref, top_s, mix_s):
        top_s[...] = jnp.full(top_s.shape, NEG, F32)
        mix_s[...] = jnp.zeros(mix_s.shape, F32)
        ones = jnp.ones((8, BLOCK), BF)

        def block(j, masked):
            here = pl.ds(pl.multiple_of(j * BLOCK, BLOCK), BLOCK)
            keys = k_ref[0, here, :]
            scores = [_dot(keys, q_ref[n], 1, 1) for n in range(HEADS)]
            weights, keeps = [], []
            for n, s in enumerate(scores):
                at = slice(n * BLOCK, (n + 1) * BLOCK)
                if masked:
                    s = jnp.where(_gap(BLOCK) >= 0, s, HIDDEN)
                old = top_s[:, at]
                top = jnp.maximum(old, s.max(axis=0, keepdims=True))
                top_s[:, at] = top
                weights.append(jnp.exp2((s - top) * e).astype(BF))
                keeps.append(jnp.exp2((old - top) * e))
            values = jnp.concatenate([v_ref[0, here, :].T, ones], axis=0)
            for n in range(HEADS):
                at = slice(n * BLOCK, (n + 1) * BLOCK)
                mix_s[:, at] = mix_s[:, at] * keeps[n] + _dot(values, weights[n], 1, 0)

        lax.fori_loop(0, i, lambda j, _: block(j, False), None)
        block(i, True)
        for n in range(HEADS):
            at = slice(n * BLOCK, (n + 1) * BLOCK)
            total = mix_s[HEAD : HEAD + 1, at]
            o_ref[n] = (mix_s[:HEAD, at] * (1 / total)).T.astype(BF)
            lse_ref[n : n + 1, :] = top_s[:, at] * scale + jnp.log(total)

    return _call(kernel, tokens // BLOCK, (q, k, v), [_heads(HEADS), _whole(k), _whole(v)], [_heads(HEADS), _stats()],
                 [_like(*q.shape), _like(HEADS, tokens, dtype=F32)], [pltpu.VMEM((1, columns), F32), pltpu.VMEM((HEAD + 8, columns), F32)],
                 flops=3 * tokens * q.size, beside=beside)


def attend_back(q, k, v, d_out, lse, delta, beside):
    tokens = q.shape[1]
    columns = HEADS * BLOCK
    scale = HEAD**-0.5
    e = scale * LOG2E
    steps = tokens // BLOCK

    def kernel(i, q_ref, k_ref, v_ref, do_ref, lse_ref, delta_ref, dq_ref, dk_ref, dv_ref, dq_s, dk_s, dv_s):
        @pl.when(i == 0)
        def _():
            dk_s[...] = jnp.zeros(dk_s.shape, F32)
            dv_s[...] = jnp.zeros(dv_s.shape, F32)

        dq_s[...] = jnp.zeros(dq_s.shape, F32)

        def block(j, masked):
            here = pl.ds(pl.multiple_of(j * BLOCK, BLOCK), BLOCK)
            keys, values = k_ref[0, here, :], v_ref[0, here, :]
            scores = [_dot(keys, q_ref[n], 1, 1) for n in range(HEADS)]
            dps = [_dot(values, do_ref[n], 1, 1) for n in range(HEADS)]
            for n in range(HEADS):
                at = slice(n * BLOCK, (n + 1) * BLOCK)
                p = jnp.exp2(scores[n] * e - lse_ref[n : n + 1, :] * LOG2E)
                if masked:
                    p = jnp.where(_gap(BLOCK) >= 0, p, 0.0)
                ds = (p * (dps[n] - delta_ref[n : n + 1, :])).astype(BF)
                dv_s[here, :] += _dot(p.astype(BF), do_ref[n], 1, 0)
                dk_s[here, :] += _dot(ds, q_ref[n], 1, 0)
                dq_s[:, at] += _dot(keys.T, ds, 1, 0)

        lax.fori_loop(0, i, lambda j, _: block(j, False), None)
        block(i, True)
        for n in range(HEADS):
            dq_ref[n] = (dq_s[:, n * BLOCK : (n + 1) * BLOCK] * scale).T.astype(BF)

        @pl.when(i == steps - 1)
        def _():
            dk_ref[0] = (dk_s[...] * scale).astype(BF)
            dv_ref[0] = dv_s[...].astype(BF)

    return _call(kernel, steps, (q, k, v, d_out, lse, delta), [_heads(HEADS), _whole(k), _whole(v), _heads(HEADS), _stats(), _stats()],
                 [_heads(HEADS), _whole(k), _whole(v)], [_like(*q.shape), _like(*k.shape), _like(*v.shape)],
                 [pltpu.VMEM((HEAD, columns), F32), pltpu.VMEM((tokens, HEAD), F32), pltpu.VMEM((tokens, HEAD), F32)],
                 flops=6 * tokens * q.size, beside=beside)


def leave(h, o, wo):
    def kernel(i, h_ref, o_ref, wo_ref, out_ref):
        out_ref[...] = _add(h_ref[...], sum(_dot(o_ref[n], wo_ref[_part(n), :], 1, 0) for n in range(HEADS)))

    tokens, d = h.shape
    return _call(kernel, tokens // BLOCK, (h, o, wo), [_rows(d), _heads(HEADS), _whole(wo)], [_rows(d)], [_like(*h.shape)], flops=2 * tokens * wo.size)[0]


def _feed_specs(d, chunk=CHUNK):
    return [*[pl.BlockSpec((d, chunk), lambda i: (0, i))] * 2, pl.BlockSpec((chunk, d), lambda i: (i, 0))]


def feed(h, gate, up, down, beside):
    tokens, d = h.shape
    steps = down.shape[0] // CHUNK

    def kernel(i, h_ref, gate_ref, up_ref, down_ref, out_ref, b_s, sum_s):
        @pl.when(i == 0)
        def _():
            b_s[...] = _norm(h_ref[...])
            sum_s[...] = jnp.zeros(sum_s.shape, F32)

        b = b_s[...]
        g = _dot(b, gate_ref[...], 1, 0)
        u = _dot(b, up_ref[...], 1, 0)
        sum_s[...] += _dot((g * jax.nn.sigmoid(g) * u).astype(BF), down_ref[...], 1, 0)

        @pl.when(i == steps - 1)
        def _():
            out_ref[...] = _add(h_ref[...], sum_s[...])

    return _call(kernel, steps, (h, gate, up, down), [_whole(h), *_feed_specs(d)], [_whole(h)], [_like(*h.shape)],
                 [pltpu.VMEM(h.shape, BF), pltpu.VMEM(h.shape, F32)], flops=6 * tokens * down.size, beside=beside)


def feed_back(h, dy, gate, up, down, beside, chunk=CHUNK):
    tokens, d = h.shape
    hidden = down.shape[0]
    steps = hidden // chunk

    def kernel(i, h_ref, dy_ref, gate_ref, up_ref, down_ref, dh_ref, dgate_ref, dup_ref, ddown_ref, b_s, bt_s, dyt_s, sum_s):
        @pl.when(i == 0)
        def _():
            b = _norm(h_ref[...])
            b_s[...] = b
            bt_s[...] = b.T
            dyt_s[...] = dy_ref[...].T
            sum_s[...] = jnp.zeros(sum_s.shape, F32)

        b = b_s[...]
        g = _dot(b, gate_ref[...], 1, 0)
        u = _dot(b, up_ref[...], 1, 0)
        by = _dot(dy_ref[...], down_ref[...], 1, 1).astype(BF).astype(F32)
        s = jax.nn.sigmoid(g)
        silu = g * s
        p = (silu * u).astype(BF)
        du = (by * silu).astype(BF)
        dg = (by * u * (s + silu * (1 - s))).astype(BF)
        sum_s[...] += _dot(dg, gate_ref[...], 1, 1) + _dot(du, up_ref[...], 1, 1)
        dgate_ref[...] = _dot(bt_s[...], dg, 1, 0).astype(BF)
        dup_ref[...] = _dot(bt_s[...], du, 1, 0).astype(BF)
        ddown_ref[...] = _dot(dyt_s[...], p, 1, 0).T.astype(BF)

        @pl.when(i == steps - 1)
        def _():
            dh_ref[...] = _add(dy_ref[...], _norm_back(h_ref[...], sum_s[...]))

    specs = _feed_specs(d, chunk)
    return _call(kernel, steps, (h, dy, gate, up, down), [_whole(h), _whole(h), *specs], [_whole(h), *specs],
                 [_like(*h.shape), _like(d, hidden), _like(d, hidden), _like(hidden, d)],
                 [pltpu.VMEM(h.shape, BF), pltpu.VMEM((d, tokens), BF), pltpu.VMEM((d, tokens), BF), pltpu.VMEM(h.shape, F32)],
                 flops=16 * tokens * down.size, beside=beside)


def leave_back(dh, o, wo):
    tokens, d = dh.shape
    steps = tokens // BLOCK

    def kernel(i, dh_ref, o_ref, wo_ref, do_ref, delta_ref, dwo_ref, sum_s):
        dh = dh_ref[...]
        for n in range(HEADS):
            rows = _part(n)
            do = _dot(dh, wo_ref[rows, :], 1, 1).astype(BF)
            do_ref[n] = do
            o = o_ref[n]
            each = do.astype(F32) * o.astype(F32)
            each = each[:, : HEAD // 2] + each[:, HEAD // 2 :]
            delta_ref[n : n + 1, :] = jnp.sum(each.T, axis=0, keepdims=True)
            sum_s[rows, :] = jnp.where(i == 0, 0.0, sum_s[rows, :]) + _dot(o.T, dh, 1, 0)

        @pl.when(i == steps - 1)
        def _():
            dwo_ref[...] = sum_s[...].astype(BF)

    return _call(kernel, steps, (dh, o, wo), [_rows(d), _heads(HEADS), _whole(wo)], [_heads(HEADS), _stats(), _whole(wo)],
                 [_like(*o.shape), _like(HEADS, tokens, dtype=F32), _like(*wo.shape)], [pltpu.VMEM(wo.shape, F32)], flops=4 * tokens * wo.size)


def enter_back(h, dq, dk, dv, tables, dh=None, w=None):
    tokens, d = h.shape
    steps = tokens // BLOCK
    through = dh is not None
    dw = _like(d, (HEADS + 2) * HEAD)

    def kernel(i, h_ref, dq_ref, dk_ref, dv_ref, cos_ref, sin_ref, *rest):
        *rest, dw_ref, sum_s = rest
        cos, sin = cos_ref[...], -sin_ref[...]
        dt = jnp.concatenate([*[_turn(dq_ref[n], cos, sin) for n in range(HEADS)], _turn(dk_ref[0], cos, sin), dv_ref[0]], axis=1)
        h = h_ref[...]
        sum_s[...] = jnp.where(i == 0, 0.0, sum_s[...]) + _dot(_norm(h).T, dt, 1, 0)
        if through:
            dh_ref, w_ref, out_ref = rest
            out_ref[...] = _add(dh_ref[...], _norm_back(h, _dot(dt, w_ref[...], 1, 1)))

        @pl.when(i == steps - 1)
        def _():
            dw_ref[...] = sum_s[...].astype(BF)

    more = ((dh, w), [_rows(d), _whole(dw)], [_rows(d)], [_like(*h.shape)]) if through else ((), [], [], [])
    return _call(kernel, steps, (h, dq, dk, dv, *tables, *more[0]), [_rows(d), _heads(HEADS), _heads(1), _heads(1), *[_rows(HEAD // 2)] * 2, *more[1]],
                 [*more[2], _whole(dw)], [*more[3], dw], [pltpu.VMEM(dw.shape, F32)], flops=(2 + 2 * through) * tokens * dw.size)


def adamw(w, m, v, g):
    m = 0.9 * m + 0.1 * g
    v = 0.95 * v + 0.05 * g * g
    step = m * lax.rsqrt(v + 1e-8) + 0.1 * w
    return (w - 0.02 * step).astype(BF), m, v


def solution(mesh):
    def step(x, dy, *arrays):
        weights, m, v = (dict(zip(NAMES, arrays[i : i + 7], strict=True)) for i in (0, 7, 14))
        tokens, d = x.shape[1:]
        sides = [weights[name].shape[2] for name in NAMES[:3]]
        entries = [jnp.concatenate([weights[name][n] for name in NAMES[:3]], 1) for n in range(2)]
        h0 = x[0]
        tables, (entry0, wo0) = turning(tokens, Gather([entries[0], weights["wo"][0]], 0, halved=1))
        q0, k0, v0 = enter(h0, entry0, tables)
        (o0, lse0), ffn0 = attend(q0, k0, v0, Gather([weights[name][0] for name in FFN], 1, {3: [("line", 0)]}, 2))
        gate0, up0, down0 = ffn0
        mid0 = leave(h0, o0, wo0)
        rest = Gather([*(weights[name][1] for name in FFN), entries[1], weights["wo"][1]], 2,
                      {2: [("line", 0)], 3: [("line", 1), ("far", 0)], 4: [("line", 2), ("far", 1)]}, 2)
        (h1,), others = feed(mid0, gate0, up0, down0, rest)
        gate1, up1, down1, entry1, wo1 = others
        q1, k1, v1 = enter(h1, entry1, tables)
        o1, lse1 = attend(q1, k1, v1, Nothing())
        mid1 = leave(h1, o1, wo1)

        by, d_gate, d_up, d_down = feed_back(mid1, dy[0], gate1, up1, down1, Nothing())
        new = [{}, {}]
        d_o, delta, d_wo1 = leave_back(by, o1, wo1)
        dq, dk, dv = attend_back(q1, k1, v1, d_o, lse1, delta, Nothing())
        by, d_entry1 = enter_back(h1, dq, dk, dv, tables, by, entry1)
        ones = {0: [0, 1], 1: [2, 3, 4], 2: [5, 6]}
        twos = {2: [0], 3: [1], 4: [2], 5: [3], 7: [4], 8: [5], 9: [6]}
        plan = {at: [("one", i) for i in ones.get(at, ())] + [("two", i) for i in twos.get(at, ())] for at in range(10)}
        plan[3] += [("one", 7), ("one", 8)]
        (by, *d_ffn), sums = feed_back(mid0, by, gate0, up0, down0, Scatter([d_gate, d_up, d_down, d_entry1, d_wo1], 5, plan), CHUNK // 2)
        *sums, entry_sum1, new[1]["wo"] = sums
        new[1].update(zip(FFN, sums))
        d_o, delta, d_wo0 = leave_back(by, o0, wo0)
        (dq, dk, dv), sums = attend_back(q0, k0, v0, d_o, lse0, delta, Scatter([*d_ffn, d_wo0], 3, {1: [("one", 0), ("one", 1)], 2: [("one", 2)], 3: [("one", 3), ("two", 0)]}))
        (d_entry0,) = enter_back(h0, dq, dk, dv, tables)
        *sums, new[0]["wo"] = sums
        new[0].update(zip(FFN, sums))
        (entry_sum0,) = alone(Scatter([d_entry0], 4))

        for n, g in enumerate((entry_sum0, entry_sum1)):
            at = 0
            for name, size in zip(NAMES, sides):
                new[n][name] = g[:, at : at + size]
                at += size
        out = [adamw(weights[name].astype(F32), m[name], v[name], jnp.stack([one[name] for one in new]).astype(F32)) for name in NAMES]
        return tuple(one[which] for which in range(3) for one in out)

    states, cut = P(("rep", "dp"), None, None), P(None, "dp", None)
    return jax.shard_map(
        step,
        mesh=mesh,
        in_specs=(states, states) + (cut,) * 21,
        out_specs=(P("rep", "dp", None),) * 21,
        check_vma=False,
    )
```
